256 devices in a mesh: dp: 2 (over core), ret: 16 (over y, x), ctx: 8 (over z).
Axes of the slice: x: 4, y: 4, z: 8, core: 2. Of those that a mesh axis runs over, the one named last changes fastest.
Arguments:
- queries: bfloat16 [2, 8192, 4096], P('dp', 'ret', 'ctx'), may hold values from -6 to 6
- enc_states: bfloat16 [2, 32768, 896], P('dp', 'ret'), may hold values from -1600 to 1600
- w_key: bfloat16 [896, 4096], P(None, 'ctx'), may hold values from -0.1875 to 0.1875
- w_value: bfloat16 [896, 4096], P(None, 'ctx'), may hold values from -0.59765625 to 0.59765625
- shard_ids: int32 [2, 128, 2], P('dp', 'ret'), may hold values from 0 to 15, all different within a row; in each aligned block of 8 rows (0 to 7, 8 to 15, ..., all dimensions but the last counted through in order) at most 2 rows name the same one
- row_ids: int32 [2, 128, 2], P('dp', 'ret'), may hold values from 0 to 15
- grad_out: bfloat16 [2, 8192, 4096], P('dp', 'ret', 'ctx'), may hold values from -6 to 6
Outputs:
- attended: bfloat16 [2, 8192, 4096], P('dp', 'ret', 'ctx')
- grad_queries: bfloat16 [2, 8192, 4096], P('dp', 'ret', 'ctx')
- grad_w_key: float32 [896, 4096], P(('dp', 'ret'), 'ctx')
- grad_w_value: float32 [896, 4096], P(('dp', 'ret'), 'ctx')
The draws below stay inside these ranges and needn't reach their ends.
Inputs may be any that keep to these rules, and one draw needn't show every extreme that they name: `shard_ids`: each block names 2 different shards; among the 8 blocks that one index of ret holds, no shard is named by more than 2 blocks, a bound that some block reaches.
All inputs are finite; a program needn't handle non-finite values.
Results may differ from the reference program's by a relative error of at most 0.019.
Values may be sent and summed in bfloat16 or wider, within the bound.
A program may use at most 128 MiB of HBM per device.

```python
import math
import jax
import jax.numpy as jnp
import numpy as np
from jax import lax

HEADS = 32
HEAD_DIM = 128
ENC_WIDTH = 896
BLOCK_LEN = 64
NEIGH_LEN = 128
NEIGHBOURS = 2
BLOCKS_DEV = 8
DB_DEV = 16
CAPACITY = 2
BATCH = 2
BLOCKS = 128
SEQ_LEN = 8192
N_RET = 16


def draw_queries(key, part):
    second = jax.random.fold_in(key, 1)
    shape = (BATCH, SEQ_LEN, HEADS * HEAD_DIM)
    base = jnp.clip(jax.random.normal(second, shape, jnp.float32), -4.0, 4.0) * 1.5
    return base.astype(jnp.bfloat16)


def draw_enc_states(key, part):
    keys_list = jax.random.split(key, 6)
    db_rows = N_RET * DB_DEV * NEIGH_LEN
    shape = (BATCH, db_rows, ENC_WIDTH)
    row_scale = jnp.exp(jax.random.uniform(keys_list[0], (BATCH, db_rows, 1), jnp.float32, 0.0, math.log(10.0)))
    col_scale = jnp.exp(jax.random.uniform(keys_list[1], (BATCH, 1, ENC_WIDTH), jnp.float32, 0.0, math.log(10.0)))
    block_total = BATCH * N_RET
    pairing = jax.random.permutation(keys_list[2], block_total)
    batch_index = jnp.arange(BATCH, dtype=jnp.int32)[:, None, None]
    row_index = jnp.arange(db_rows, dtype=jnp.int32)[None, :, None]
    row_block = batch_index * N_RET + row_index // (DB_DEV * NEIGH_LEN)
    col_block = (jnp.arange(ENC_WIDTH, dtype=jnp.int32) // (ENC_WIDTH // block_total))[None, None, :]
    spike = jnp.where(pairing[row_block] == col_block, 4.0, 1.0)
    base = jnp.clip(jax.random.normal(keys_list[5], shape, jnp.float32), -4.0, 4.0)
    return (base * row_scale * col_scale * spike).astype(jnp.bfloat16)


def with_ends(array, rng, smallest, top_value):
    dims = array.shape
    index_at = [jax.random.randint(jax.random.fold_in(rng, axis), (), 0, dims[axis]) for axis in range(len(dims))]
    array = array.at[tuple(index_at)].set(smallest)
    longest = dims.index(max(dims))
    index_at[longest] = (index_at[longest] + 1) % dims[longest]
    return array.at[tuple(index_at)].set(top_value)


def shard_levels(own_key, extent, cuts, low, top_value):
    factor_of = 1.0
    for position, blocks in cuts:
        heights = jax.random.uniform(jax.random.fold_in(jax.random.fold_in(own_key, 6), position), (blocks,), jnp.float32, low / len(cuts), top_value / len(cuts))
        factor_of = factor_of * jnp.repeat(jnp.exp(heights), extent[position] // blocks).reshape((-1,) + (1,) * (len(extent) - 1 - position))
    return factor_of


def deal_out(stream_key, own, number, rows, count, top, limit, skew):
    order = jax.random.permutation(stream_key, count)
    crowded, ordinary = shares(count, rows * top, limit, skew, True), shares(count, rows * top, limit, skew, False)
    places = jnp.arange(count)

    def named(lengths, turn):
        used = int((lengths > 0).sum())
        fixed = max(1, used // 4)
        shifted = fixed + (places - fixed + turn * (used - fixed)) % max(1, count - fixed)
        return jnp.zeros((count,), jnp.int32).at[order[jnp.where(places < fixed, places, shifted)]].set(jnp.asarray(lengths, jnp.int32))

    lengths = jnp.where(number % 4 == 0, named(crowded, number // 4), named(ordinary, number - number // 4 - 1))
    mixed = jax.random.permutation(jax.random.fold_in(own, 3), count)
    giver, sink = mixed[0:count // 2 * 2:2], mixed[1:count // 2 * 2:2]
    slack = jnp.minimum(lengths[giver] - 1, limit - lengths[sink]) // 2
    slack = jnp.where((giver == order[0]) | (sink == order[0]) | (lengths[sink] == 0), 0, jnp.maximum(slack, 0))
    shifted = jax.random.randint(jax.random.fold_in(own, 4), (count // 2,), 0, 1 << 20) % (slack + 1)
    lengths = lengths.at[giver].add(-shifted).at[sink].add(shifted)
    members = jnp.searchsorted(jnp.cumsum(lengths), jnp.arange(rows * top), side="right").astype(jnp.int32)
    listing = members.reshape(top, rows).T
    listing = listing[jax.random.permutation(jax.random.fold_in(own, 1), rows)]
    turn = jax.random.randint(jax.random.fold_in(own, 2), (rows, 1), 0, top)
    return jnp.take_along_axis(listing, (jnp.arange(top)[None, :] + turn) % top, axis=1)


def shares(count, total, reach, slope, full):
    portions = [(1 << 20) // math.isqrt(rank ** slope) + 1 for rank in range(1, count + 1)]
    largest = reach if full else min(reach, max(-(-total // count), total * portions[0] // sum(portions)))
    least = 1 if total - largest >= count - 1 else 0
    holding, rest = [largest] + [least] * (count - 1), total - largest - least * (count - 1)
    while rest > 0:
        candidates = [i for i in range(1, count) if holding[i] < largest] or [i for i in range(1, count) if holding[i] < reach]
        pool, budget = sum([portions[i] for i in candidates]), rest
        for i in candidates:
            more = min(reach - holding[i], max(1, budget * portions[i] // pool), rest)
            holding[i] = holding[i] + more
            rest = rest - more
    return np.array(holding)


def noise(key, dims, scale, reach, pieces=(), kind=jnp.bfloat16):
    gain = shard_levels(key, dims, pieces, -0.22, 0.18) if pieces else 1.0
    drawn = jax.random.normal(key, dims, jnp.float32) * scale * gain
    return jnp.minimum(jnp.maximum(drawn, -reach), reach).astype(kind)


def setup_inputs(seed: int = 0) -> dict:
    seeds = jax.random.split(jax.random.key(seed), 8)
    queries = draw_queries(jax.random.fold_in(seeds[7], 71), 0)
    enc_states = draw_enc_states(jax.random.fold_in(seeds[7], 71), 0)
    w_key = noise(seeds[2], (ENC_WIDTH, HEADS * HEAD_DIM), ENC_WIDTH ** -0.5, 0.1875, ((1, 8),))
    w_value = noise(seeds[3], (ENC_WIDTH, HEADS * HEAD_DIM), (3.0 / ENC_WIDTH ** 0.5), 0.59765625, ((1, 8),))
    shard_ids_keys = jax.random.split(jax.random.fold_in(seeds[4], 1), BATCH * BLOCKS // BLOCKS_DEV)
    shard_ids_turns = jax.random.permutation(jax.random.fold_in(seeds[4], 3), BATCH * BLOCKS // BLOCKS_DEV)
    shard_ids = jax.vmap(lambda own, number: deal_out(jax.random.fold_in(seeds[4], 2), own, number, BLOCKS_DEV, N_RET, NEIGHBOURS, CAPACITY, 2))(shard_ids_keys, shard_ids_turns).reshape((BATCH, BLOCKS, NEIGHBOURS))
    row_ids = with_ends(jax.random.randint(seeds[5], (BATCH, BLOCKS, NEIGHBOURS), 0, DB_DEV), jax.random.fold_in(seeds[5], 1), 0, DB_DEV - 1).astype(jnp.int32)
    grad_out = noise(seeds[6], (BATCH, SEQ_LEN, HEADS * HEAD_DIM), 1.0, 6.0, ((0, 2), (1, 16), (2, 8)))
    return dict(queries=queries, enc_states=enc_states, w_key=w_key, w_value=w_value, shard_ids=shard_ids, row_ids=row_ids, grad_out=grad_out)


def rounded(tensor):
    return lax.optimization_barrier(tensor.astype(jnp.bfloat16)).astype(jnp.float32)

def normalize_rows(states):
    floats = states.astype(jnp.float32)
    mean_square = lax.optimization_barrier(jnp.mean(floats * floats, axis=-1, keepdims=True))
    return (floats * lax.rsqrt(mean_square + 1e-06)).astype(jnp.bfloat16)

def contract_rows(lhs_rows, rhs_rows):
    return lax.dot_general(lhs_rows, rhs_rows, (((0,), (0,)), ((), ())), preferred_element_type=jnp.float32)

def block_attention(query_block, key_block, value_block, grad_block):
    score_scale = 1.0 / math.sqrt(HEAD_DIM)
    query_f = query_block.astype(jnp.float32)
    key_f = key_block.astype(jnp.float32)
    value_f = value_block.astype(jnp.float32)
    grad_f = grad_block.astype(jnp.float32)
    scores = jnp.einsum('thd,jhd->htj', query_f, key_f) * score_scale
    exponent = jnp.exp(scores)
    denominator = lax.optimization_barrier(jnp.sum(exponent, axis=-1))
    numerator = jnp.einsum('htj,jhd->thd', rounded(exponent), value_f)
    output = numerator / jnp.transpose(denominator)[:, :, None]
    prob_grad = jnp.einsum('thd,jhd->htj', grad_f, value_f)
    row_delta = jnp.transpose(lax.optimization_barrier(jnp.sum(grad_f * output, axis=-1)))
    probability = exponent / denominator[:, :, None]
    score_grad = rounded(probability * (prob_grad - row_delta[:, :, None]) * score_scale)
    grad_query = jnp.einsum('htj,jhd->thd', score_grad, key_f).astype(jnp.bfloat16)
    grad_key = jnp.einsum('htj,thd->jhd', score_grad, query_f).astype(jnp.bfloat16)
    grad_value = jnp.einsum('htj,thd->jhd', rounded(probability), grad_f).astype(jnp.bfloat16)
    return (output.astype(jnp.bfloat16), grad_query, grad_key, grad_value)

def reference(queries, enc_states, w_key, w_value, shard_ids, row_ids, grad_out):
    feat_width = HEADS * HEAD_DIM
    context_rows = NEIGHBOURS * NEIGH_LEN
    attended_list = []
    grad_list = []
    sum_key = jnp.zeros((ENC_WIDTH, feat_width), jnp.float32)
    sum_value = jnp.zeros((ENC_WIDTH, feat_width), jnp.float32)
    for replica in range(queries.shape[0]):
        normed = lax.optimization_barrier(normalize_rows(enc_states[replica]))
        key_table = lax.optimization_barrier(jnp.dot(normed, w_key, preferred_element_type=jnp.float32).astype(jnp.bfloat16)).reshape(N_RET * DB_DEV, NEIGH_LEN, HEADS, HEAD_DIM)
        value_table = lax.optimization_barrier(jnp.dot(normed, w_value, preferred_element_type=jnp.float32).astype(jnp.bfloat16)).reshape(N_RET * DB_DEV, NEIGH_LEN, HEADS, HEAD_DIM)
        normed_table = normed.reshape(N_RET * DB_DEV, NEIGH_LEN, ENC_WIDTH)
        neighbour = (shard_ids[replica] * DB_DEV + row_ids[replica]).astype(jnp.int32)
        query_blocks = queries[replica].reshape(BLOCKS, BLOCK_LEN, HEADS, HEAD_DIM)
        grad_blocks = grad_out[replica].reshape(BLOCKS, BLOCK_LEN, HEADS, HEAD_DIM)

        def block_step(running, inputs):
            query_block, grad_block, chosen = inputs
            key_block = key_table[chosen].reshape(context_rows, HEADS, HEAD_DIM)
            value_block = value_table[chosen].reshape(context_rows, HEADS, HEAD_DIM)
            output, grad_query, grad_key, grad_value = block_attention(query_block, key_block, value_block, grad_block)
            state_rows = normed_table[chosen].reshape(context_rows, ENC_WIDTH)
            key_sum = running[0] + contract_rows(state_rows, grad_key.reshape(context_rows, feat_width))
            value_sum = running[1] + contract_rows(state_rows, grad_value.reshape(context_rows, feat_width))
            return ((key_sum, value_sum), (output, grad_query))
        (sum_key, sum_value), (outputs, grads) = lax.scan(block_step, (sum_key, sum_value), (query_blocks, grad_blocks, neighbour))
        attended_list.append(outputs.reshape(SEQ_LEN, feat_width))
        grad_list.append(grads.reshape(SEQ_LEN, feat_width))
    return (jnp.stack(attended_list), jnp.stack(grad_list), sum_key, sum_value)
```

```python
import functools
import math

import jax
import jax.numpy as jnp
from jax import lax
from jax.experimental import pallas as pl
from jax.experimental.pallas import tpu as pltpu
from jax.sharding import PartitionSpec as P

HEAD_DIM = 128
NEIGH_LEN = 128
NEIGHBOURS = 2
CAPACITY = 2
MESH = pl.DeviceIdType.MESH
VMEM_LIMIT = 60 * 1024 * 1024


def normalize_rows(states):
    floats = states.astype(jnp.float32)
    mean_square = jnp.mean(floats * floats, axis=-1, keepdims=True)
    return (floats * lax.rsqrt(mean_square + 1e-06)).astype(jnp.bfloat16)


def gather_kernel(
    n_ret, n_ctx, chunks, shard_ref, row_ref, enc_ref, ctx_ref,
    table, arrived, picks, piece, outbound, landed,
    local_sem, table_send, table_recv, slot_send, slot_recv, ring_send, ring_recv,
):
    me = lax.axis_index("ret")
    plane = lax.axis_index("ctx")
    requests = ctx_ref.shape[1]
    rows = piece.shape[1]
    up, down = lax.rem(plane + 1, n_ctx), lax.rem(plane + n_ctx - 1, n_ctx)

    barrier = pltpu.get_barrier_semaphore()

    @pl.loop(1, n_ret)
    def _(k):
        pl.semaphore_signal(
            barrier, inc=1, device_id={"ret": lax.rem(me + k, n_ret)}, device_id_type=MESH
        )

    for z in (up, down):
        pl.semaphore_signal(barrier, inc=1, device_id={"ctx": z}, device_id_type=MESH)

    fetch = pltpu.make_async_copy(
        enc_ref.at[:, pl.ds(pl.multiple_of(plane * rows, rows), rows), :], piece, local_sem.at[0]
    )
    fetch.start()

    shards = [shard_ref[i // NEIGHBOURS, i % NEIGHBOURS] for i in range(requests)]
    slots = []
    for i in range(requests):
        rank = jnp.int32(0)
        for j in range(i):
            if j // NEIGHBOURS != i // NEIGHBOURS:
                rank = rank + jnp.where(shards[j] == shards[i], 1, 0)
        slots.append(shards[i] * CAPACITY + jnp.minimum(rank, CAPACITY - 1))
    shape = table.shape
    lane = lax.broadcasted_iota(jnp.int32, shape, 2)
    place = lax.broadcasted_iota(jnp.int32, shape, 0) * CAPACITY + lane
    place = jnp.where(lane < CAPACITY, place, -1)
    filled = jnp.zeros(shape, jnp.int32)
    for i in range(requests):
        filled = jnp.where(place == slots[i], row_ref[i // NEIGHBOURS, i % NEIGHBOURS], filled)
    table[...] = filled
    pl.semaphore_wait(barrier, n_ret - 1 + 2)

    def table_copy(k):
        peer = lax.rem(me + k, n_ret)
        return pltpu.make_async_remote_copy(
            table.at[peer], arrived.at[me], table_send.at[k], table_recv.at[k],
            device_id={"ret": peer}, device_id_type=MESH,
        )

    def slot_copy(k):
        peer = lax.rem(me + k, n_ret)
        return pltpu.make_async_remote_copy(
            outbound.at[peer], landed.at[pl.ds(me * CAPACITY, CAPACITY)],
            slot_send.at[k], slot_recv.at[k],
            device_id={"ret": peer}, device_id_type=MESH,
        )

    @pl.loop(1, n_ret)
    def _(k):
        table_copy(k).start()

    fetch.wait()

    @pl.loop(0, piece.shape[0])
    def _(i):
        piece[i] = normalize_rows(piece[i])

    @pl.loop(1, n_ret)
    def _(k):
        table_copy(k).wait()

    arrived[me] = table[me]
    to_scalars = pltpu.make_async_copy(arrived, picks, local_sem.at[1])
    to_scalars.start()
    to_scalars.wait()

    @pl.loop(1, n_ret)
    def _(k):
        peer = lax.rem(me + k, n_ret)
        for c in range(CAPACITY):
            outbound[peer, c] = piece[picks[peer, 0, c]]
        slot_copy(k).start()

    for c in range(CAPACITY):
        landed[me * CAPACITY + c] = piece[picks[me, 0, c]]

    @pl.loop(1, n_ret)
    def _(k):
        slot_copy(k).wait()

    for i in range(requests):
        ctx_ref[plane, i] = landed[slots[i]]

    size = requests // chunks

    def ring_copy(direction, chunk, hop):
        origin = lax.rem(plane + n_ctx - hop, n_ctx) if direction == 0 else lax.rem(plane + hop, n_ctx)
        where = ctx_ref.at[origin, pl.ds(chunk * size, size)]
        return pltpu.make_async_remote_copy(
            where, where,
            ring_send.at[direction, chunk, hop], ring_recv.at[direction, chunk, hop],
            device_id={"ctx": up if direction == 0 else down}, device_id_type=MESH,
        )

    half = n_ctx // 2
    hops = [[half - chunk % 2, n_ctx - 1 - half + chunk % 2] for chunk in range(chunks)]
    for wave in range(chunks + half):
        for chunk in range(chunks):
            hop = wave - chunk
            for direction in range(2):
                if hop >= 1 and hop <= hops[chunk][direction]:
                    ring_copy(direction, chunk, hop - 1).wait_recv()
                if hop >= 0 and hop < hops[chunk][direction]:
                    ring_copy(direction, chunk, hop).start()
    for chunk in range(chunks):
        for direction in range(2):
            for hop in range(hops[chunk][direction]):
                ring_copy(direction, chunk, hop).wait_send()


def gather_context(shard_ids, row_ids, enc, n_ret, n_ctx):
    db_dev, length, width = enc.shape
    requests = shard_ids.shape[0] * NEIGHBOURS
    rows = length // n_ctx
    chunks = 4
    hop_max = n_ctx // 2
    dma = pltpu.SemaphoreType.DMA
    return pl.pallas_call(
        functools.partial(gather_kernel, n_ret, n_ctx, chunks),
        out_shape=jax.ShapeDtypeStruct((n_ctx, requests, rows, width), jnp.bfloat16),
        in_specs=[
            pl.BlockSpec(memory_space=pltpu.SMEM),
            pl.BlockSpec(memory_space=pltpu.SMEM),
            pl.BlockSpec(memory_space=pl.ANY),
        ],
        out_specs=pl.BlockSpec(memory_space=pltpu.VMEM),
        scratch_shapes=[
            pltpu.VMEM((n_ret, 1, 128), jnp.int32),
            pltpu.VMEM((n_ret, 1, 128), jnp.int32),
            pltpu.SMEM((n_ret, 1, 128), jnp.int32),
            pltpu.VMEM((db_dev, rows, width), jnp.bfloat16),
            pltpu.VMEM((n_ret, CAPACITY, rows, width), jnp.bfloat16),
            pltpu.VMEM((n_ret * CAPACITY, rows, width), jnp.bfloat16),
            dma((2,)),
            dma((n_ret,)), dma((n_ret,)),
            dma((n_ret,)), dma((n_ret,)),
            dma((2, chunks, hop_max)), dma((2, chunks, hop_max)),
        ],
        compiler_params=pltpu.CompilerParams(
            collective_id=0, has_side_effects=True, vmem_limit_bytes=VMEM_LIMIT
        ),
    )(shard_ids, row_ids, enc)


def dot_nt(a, b):
    return lax.dot_general(a, b, (((1,), (1,)), ((), ())), preferred_element_type=jnp.float32)


def dot_tn(a, b):
    return lax.dot_general(a, b, (((0,), (0,)), ((), ())), preferred_element_type=jnp.float32)


def dot_nn(a, b):
    return jnp.dot(a, b, preferred_element_type=jnp.float32)


def attend_kernel(
    tokens, ctx_ref, wk_ref, wv_ref, q_ref, g_ref, att_ref, dq_ref, gw_ref, flipped, kv_grad
):
    scale = 1.0 / math.sqrt(HEAD_DIM)
    blocks = q_ref.shape[0] // tokens
    width = ctx_ref.shape[3]
    feat = q_ref.shape[1]
    context = NEIGHBOURS * NEIGH_LEN
    pair = 2 * HEAD_DIM

    def stacked(x):
        lane = lax.broadcasted_iota(jnp.int32, x.shape, 1)
        zero = jnp.zeros_like(x)
        return jnp.concatenate(
            [jnp.where(lane < HEAD_DIM, x, zero), jnp.where(lane >= HEAD_DIM, x, zero)], axis=0
        )

    def unstacked(x):
        return jnp.concatenate([x[:tokens, :HEAD_DIM], x[tokens:, HEAD_DIM:]], axis=1)

    @pl.loop(0, blocks)
    def _(u):
        normed = ctx_ref[:, pl.ds(u * NEIGHBOURS, NEIGHBOURS)].reshape(context, width)
        at = pl.ds(pl.multiple_of(u * context, context), context)
        flipped[:, at] = normed.T
        rows = pl.ds(pl.multiple_of(u * tokens, tokens), tokens)
        for p in range(feat // pair):
            cols = pl.ds(p * pair, pair)
            keys = dot_nn(normed, wk_ref[:, cols]).astype(jnp.bfloat16)
            values = dot_nn(normed, wv_ref[:, cols]).astype(jnp.bfloat16)
            q = stacked(q_ref[rows, cols])
            g = stacked(g_ref[rows, cols])
            expo = jnp.exp(dot_nt(q, keys) * scale)
            inverse = 1.0 / jnp.sum(expo, axis=1, keepdims=True)
            out = dot_nn(expo.astype(jnp.bfloat16), values) * inverse
            att_ref[rows, cols] = unstacked(out).astype(jnp.bfloat16)
            delta = jnp.sum(g.astype(jnp.float32) * out, axis=1, keepdims=True)
            dprob = dot_nt(g, values)
            probs = expo * inverse
            dscore = (probs * (dprob - delta) * scale).astype(jnp.bfloat16)
            dq_ref[rows, cols] = unstacked(dot_nn(dscore, keys)).astype(jnp.bfloat16)
            kv_grad[at, cols] = dot_tn(dscore, q).astype(jnp.bfloat16)
            kv_grad[at, pl.ds(feat + p * pair, pair)] = dot_tn(
                probs.astype(jnp.bfloat16), g
            ).astype(jnp.bfloat16)

    tile = 64

    @pl.loop(0, width // 2 // tile)
    def _(i):
        at = pl.ds(pl.multiple_of(i * tile, tile), tile)
        for part in range(2):
            whole = pl.ds(pl.multiple_of(part * (width // 2) + i * tile, tile), tile)
            gw_ref[part, at, :] = dot_nn(flipped[whole, :], kv_grad[...])


def attend(ctx, w_key, w_value, queries, grad_out, tokens):
    n_ctx, requests, rows, width = ctx.shape
    seq, feat = queries.shape
    vmem = pl.BlockSpec(memory_space=pltpu.VMEM)
    return pl.pallas_call(
        functools.partial(attend_kernel, tokens),
        out_shape=(
            jax.ShapeDtypeStruct((seq, feat), jnp.bfloat16),
            jax.ShapeDtypeStruct((seq, feat), jnp.bfloat16),
            jax.ShapeDtypeStruct((2, width // 2, 2 * feat), jnp.float32),
        ),
        in_specs=[vmem] * 5,
        out_specs=(vmem,) * 3,
        scratch_shapes=[
            pltpu.VMEM((width, requests * NEIGH_LEN), jnp.bfloat16),
            pltpu.VMEM((requests * NEIGH_LEN, 2 * feat), jnp.bfloat16),
        ],
        compiler_params=pltpu.CompilerParams(vmem_limit_bytes=VMEM_LIMIT),
    )(ctx, w_key, w_value, queries, grad_out)


def reduce_kernel(
    n_ret, gw_ref, key_ref, value_ref,
    mine, theirs, summed, parts, landed, pair_sem, send_sem, recv_sem,
):
    me = lax.axis_index("ret")
    core = lax.axis_index("dp")
    _, half, cols = gw_ref.shape
    share = half // n_ret
    feat = cols // 2

    barrier = pltpu.get_barrier_semaphore()

    @pl.loop(1, n_ret)
    def _(k):
        pl.semaphore_signal(
            barrier, inc=1, device_id={"ret": lax.rem(me + k, n_ret)}, device_id_type=MESH
        )

    pl.semaphore_signal(barrier, inc=1, device_id={"dp": 1 - core}, device_id_type=MESH)
    mine[...] = gw_ref[1 - core].astype(jnp.bfloat16)
    pl.semaphore_wait(barrier, n_ret)
    swap = pltpu.make_async_remote_copy(
        mine, theirs, pair_sem.at[0], pair_sem.at[1],
        device_id={"dp": 1 - core}, device_id_type=MESH,
    )
    swap.start()
    swap.wait()

    def copy(k):
        peer = lax.rem(me + k, n_ret)
        return pltpu.make_async_remote_copy(
            parts.at[peer], landed.at[k], send_sem.at[k], recv_sem.at[k],
            device_id={"ret": peer}, device_id_type=MESH,
        )

    summed[...] = gw_ref[core] + theirs[...].astype(jnp.float32)
    for r in range(n_ret):
        parts[r, :share, :] = summed[pl.ds(r * share, share), :].astype(jnp.bfloat16)

    @pl.loop(1, n_ret)
    def _(k):
        copy(k).start()

    landed[0] = parts[me]

    @pl.loop(1, n_ret)
    def _(k):
        copy(k).wait()

    total = landed[0, :share, :].astype(jnp.float32)
    for k in range(1, n_ret):
        total = total + landed[k, :share, :].astype(jnp.float32)
    key_ref[...] = total[:, :feat]
    value_ref[...] = total[:, feat:]


def reduce_grads(gw, n_ret):
    _, half, cols = gw.shape
    share = half // n_ret
    padded = -(-share // 16) * 16
    vmem = pl.BlockSpec(memory_space=pltpu.VMEM)
    dma = pltpu.SemaphoreType.DMA
    return pl.pallas_call(
        functools.partial(reduce_kernel, n_ret),
        out_shape=(jax.ShapeDtypeStruct((share, cols // 2), jnp.float32),) * 2,
        in_specs=[vmem],
        out_specs=(vmem, vmem),
        scratch_shapes=[
            pltpu.VMEM((half, cols), jnp.bfloat16),
            pltpu.VMEM((half, cols), jnp.bfloat16),
            pltpu.VMEM((half, cols), jnp.float32),
            pltpu.VMEM((n_ret, padded, cols), jnp.bfloat16),
            pltpu.VMEM((n_ret, padded, cols), jnp.bfloat16),
            dma((2,)), dma((n_ret,)), dma((n_ret,)),
        ],
        compiler_params=pltpu.CompilerParams(
            collective_id=1, has_side_effects=True, vmem_limit_bytes=VMEM_LIMIT
        ),
    )(gw)


def solution(mesh):
    n_ret, n_ctx = mesh.shape["ret"], mesh.shape["ctx"]

    def local(queries, enc_states, w_key, w_value, shard_ids, row_ids, grad_out):
        enc = enc_states[0].reshape(-1, NEIGH_LEN, enc_states.shape[2])
        tokens = queries.shape[1] // shard_ids.shape[1]
        ctx = gather_context(shard_ids[0], row_ids[0], enc, n_ret, n_ctx)
        attended, grad_queries, gw = attend(ctx, w_key, w_value, queries[0], grad_out[0], tokens)
        grad_key, grad_value = reduce_grads(gw, n_ret)
        return attended[None], grad_queries[None], grad_key, grad_value

    spread = P("dp", "ret", "ctx")
    listed = P("dp", "ret", None)
    return jax.shard_map(
        local,
        mesh=mesh,
        in_specs=(spread, listed, P(None, "ctx"), P(None, "ctx"), listed, listed, spread),
        out_specs=(spread, spread, P(("dp", "ret"), "ctx"), P(("dp", "ret"), "ctx")),
        check_vma=False,
    )
```

```python
import functools
import math

import jax
import jax.numpy as jnp
from jax import lax
from jax.experimental import pallas as pl
from jax.experimental.pallas import tpu as pltpu
from jax.sharding import PartitionSpec as P

HEAD_DIM = 128
NEIGH_LEN = 128
NEIGHBOURS = 2
CAPACITY = 2
MESH = pl.DeviceIdType.MESH
VMEM_LIMIT = 60 * 1024 * 1024
PAIR = 2 * HEAD_DIM
CHUNKS = 4


def normalize_rows(states):
    floats = states.astype(jnp.float32)
    mean_square = jnp.mean(floats * floats, axis=-1, keepdims=True)
    return (floats * lax.rsqrt(mean_square + 1e-06)).astype(jnp.bfloat16)


def dot_nt(a, b):
    return lax.dot_general(a, b, (((1,), (1,)), ((), ())), preferred_element_type=jnp.float32)


def dot_tn(a, b):
    return lax.dot_general(a, b, (((0,), (0,)), ((), ())), preferred_element_type=jnp.float32)


def dot_nn(a, b):
    return jnp.dot(a, b, preferred_element_type=jnp.float32)


def stacked(x):
    lane = lax.broadcasted_iota(jnp.int32, x.shape, 1)
    zero = jnp.zeros_like(x)
    return jnp.concatenate(
        [jnp.where(lane < HEAD_DIM, x, zero), jnp.where(lane >= HEAD_DIM, x, zero)], axis=0
    )


def unstacked(x):
    tokens = x.shape[0] // 2
    return jnp.concatenate([x[:tokens, :HEAD_DIM], x[tokens:, HEAD_DIM:]], axis=1)


def attend_pair(q, g, keys, values):
    scale = 1.0 / math.sqrt(HEAD_DIM)
    q, g = stacked(q), stacked(g)
    expo = jnp.exp(dot_nt(q, keys) * scale)
    inverse = 1.0 / jnp.sum(expo, axis=1, keepdims=True)
    out = dot_nn(expo.astype(jnp.bfloat16), values) * inverse
    delta = jnp.sum(g.astype(jnp.float32) * out, axis=1, keepdims=True)
    probs = expo * inverse
    dscore = (probs * (dot_nt(g, values) - delta) * scale).astype(jnp.bfloat16)
    grad_q = dot_nn(dscore, keys)
    grad_k = dot_tn(dscore, q)
    grad_v = dot_tn(probs.astype(jnp.bfloat16), g)
    return [
        x.astype(jnp.bfloat16) for x in (unstacked(out), unstacked(grad_q), grad_k, grad_v)
    ]


def step_kernel(
    n_ret, n_ctx, shard_ref, row_ref, enc_ref, wk_ref, wv_ref, q_hbm, g_hbm,
    att_ref, dq_ref, gathered,
    table, arrived, picks, piece, outbound, landed, ctx_ref, weights, q_ref, g_ref,
    projected, flipped, kv_grad, mine, theirs, summed, parts,
    local_sem, table_send, table_recv, slot_send, slot_recv, ring_send, ring_recv,
    pair_send, pair_recv, part_send, part_recv,
):
    me = lax.axis_index("ret")
    plane = lax.axis_index("ctx")
    core = lax.axis_index("dp")
    requests, rows, width = ctx_ref.shape[1:]
    feat = q_ref.shape[1]
    context = NEIGHBOURS * NEIGH_LEN
    blocks = requests // NEIGHBOURS
    tokens = q_ref.shape[0] // blocks
    up, down = lax.rem(plane + 1, n_ctx), lax.rem(plane + n_ctx - 1, n_ctx)
    sibling = {"dp": 1 - core}

    def ret_peer(k):
        return lax.rem(me + k, n_ret)

    barrier = pltpu.get_barrier_semaphore()

    @pl.loop(1, n_ret)
    def _(k):
        pl.semaphore_signal(barrier, inc=1, device_id={"ret": ret_peer(k)}, device_id_type=MESH)

    for z in (up, down):
        pl.semaphore_signal(barrier, inc=1, device_id={"ctx": z}, device_id_type=MESH)
    pl.semaphore_signal(barrier, inc=1, device_id=sibling, device_id_type=MESH)

    loads = [
        pltpu.make_async_copy(source, target, local_sem.at[i])
        for i, (source, target) in enumerate((
            (enc_ref.at[:, pl.ds(pl.multiple_of(plane * rows, rows), rows), :], piece),
            (wk_ref, weights.at[:, pl.ds(0, feat)]),
            (wv_ref, weights.at[:, pl.ds(feat, feat)]),
            (q_hbm, q_ref),
            (g_hbm, g_ref),
        ))
    ]
    for load in loads:
        load.start()

    shards = [shard_ref[i % NEIGHBOURS, i // NEIGHBOURS] for i in range(requests)]
    slots = []
    for i in range(requests):
        rank = jnp.int32(0)
        for j in range(i):
            if j // NEIGHBOURS != i // NEIGHBOURS:
                rank = rank + jnp.where(shards[j] == shards[i], 1, 0)
        slots.append(shards[i] * CAPACITY + jnp.minimum(rank, CAPACITY - 1))
    shape = table.shape
    lane = lax.broadcasted_iota(jnp.int32, shape, 2)
    place = lax.broadcasted_iota(jnp.int32, shape, 0) * CAPACITY + lane
    place = jnp.where(lane < CAPACITY, place, -1)
    filled = jnp.zeros(shape, jnp.int32)
    for i in range(requests):
        filled = jnp.where(place == slots[i], row_ref[i % NEIGHBOURS, i // NEIGHBOURS], filled)
    table[...] = filled
    pl.semaphore_wait(barrier, n_ret - 1 + 2 + 1)

    def table_copy(k):
        return pltpu.make_async_remote_copy(
            table.at[ret_peer(k)], arrived.at[me], table_send.at[k], table_recv.at[k],
            device_id={"ret": ret_peer(k)}, device_id_type=MESH,
        )

    def slot_copy(k):
        return pltpu.make_async_remote_copy(
            outbound.at[ret_peer(k)], landed.at[pl.ds(me * CAPACITY, CAPACITY)],
            slot_send.at[k], slot_recv.at[k],
            device_id={"ret": ret_peer(k)}, device_id_type=MESH,
        )

    @pl.loop(1, n_ret)
    def _(k):
        table_copy(k).start()

    loads[0].wait()

    @pl.loop(0, piece.shape[0])
    def _(i):
        piece[i] = normalize_rows(piece[i])

    @pl.loop(1, n_ret)
    def _(k):
        table_copy(k).wait()

    arrived[me] = table[me]
    to_scalars = pltpu.make_async_copy(arrived, picks, local_sem.at[5])
    to_scalars.start()
    to_scalars.wait()

    @pl.loop(1, n_ret)
    def _(k):
        peer = ret_peer(k)
        for c in range(CAPACITY):
            outbound[peer, c] = piece[picks[peer, 0, c]]
        slot_copy(k).start()

    for c in range(CAPACITY):
        landed[me * CAPACITY + c] = piece[picks[me, 0, c]]
    for load in loads[1:]:
        load.wait()

    @pl.loop(1, n_ret)
    def _(k):
        slot_copy(k).wait()

    for i in range(requests):
        ctx_ref[plane, i] = landed[slots[i]]

    size = requests // CHUNKS

    def ring_copy(direction, chunk, hop):
        step = n_ctx - hop if direction == 0 else hop
        where = ctx_ref.at[lax.rem(plane + step, n_ctx), pl.ds(chunk * size, size)]
        return pltpu.make_async_remote_copy(
            where, where,
            ring_send.at[direction, chunk, hop], ring_recv.at[direction, chunk, hop],
            device_id={"ctx": up if direction == 0 else down}, device_id_type=MESH,
        )

    def compute(chunk):
        first = chunk * size // NEIGHBOURS
        count = size // NEIGHBOURS
        normed = jnp.concatenate([
            ctx_ref[:, (first + b) * NEIGHBOURS : (first + b + 1) * NEIGHBOURS].reshape(context, width)
            for b in range(count)
        ])
        flipped[:, :, pl.ds(first * context, count * context)] = normed.T.reshape(
            2, width // 2, count * context
        )
        for p in range(2 * feat // PAIR):
            cols = pl.ds(p * PAIR, PAIR)
            projected[:, cols] = dot_nn(normed, weights[:, cols]).astype(jnp.bfloat16)
        for b in range(count):
            here = pl.ds(b * context, context)
            at = pl.ds((first + b) * context, context)
            own = pl.ds((first + b) * tokens, tokens)
            for p in range(feat // PAIR):
                cols, late = pl.ds(p * PAIR, PAIR), pl.ds(feat + p * PAIR, PAIR)
                att_ref[own, cols], dq_ref[own, cols], kv_grad[at, cols], kv_grad[at, late] = (
                    attend_pair(
                        q_ref[own, cols], g_ref[own, cols],
                        projected[here, cols], projected[here, late],
                    )
                )

    half = n_ctx // 2
    hops = [[half - chunk % 2, n_ctx - 1 - half + chunk % 2] for chunk in range(CHUNKS)]
    for wave in range(CHUNKS + half):
        for chunk in range(CHUNKS):
            hop = wave - chunk
            for direction in range(2):
                if hop >= 1 and hop <= hops[chunk][direction]:
                    ring_copy(direction, chunk, hop - 1).wait_recv()
                if hop >= 0 and hop < hops[chunk][direction]:
                    ring_copy(direction, chunk, hop).start()
        if wave >= half:
            compute(wave - half)
    for chunk in range(CHUNKS):
        for direction in range(2):
            for hop in range(hops[chunk][direction]):
                ring_copy(direction, chunk, hop).wait_send()

    tiles = 2 * feat // PAIR
    share = width // 2 // n_ret

    def pair_copy(n):
        return pltpu.make_async_remote_copy(
            mine.at[n], theirs.at[n], pair_send.at[n], pair_recv.at[n],
            device_id=sibling, device_id_type=MESH,
        )

    def part_copy(n, k):
        return pltpu.make_async_remote_copy(
            parts.at[n, ret_peer(k)], gathered.at[n, k], part_send.at[n, k], part_recv.at[n, k],
            device_id={"ret": ret_peer(k)}, device_id_type=MESH,
        )

    for n in range(tiles):
        mine[n] = dot_nn(flipped[1 - core], kv_grad[:, pl.ds(n * PAIR, PAIR)]).astype(jnp.bfloat16)
        pair_copy(n).start()
    for n in range(tiles):
        own = dot_nn(flipped[core], kv_grad[:, pl.ds(n * PAIR, PAIR)])
        pair_copy(n).wait()
        summed[...] = own + theirs[n].astype(jnp.float32)
        for r in range(n_ret):
            parts[n, r, :share, :] = summed[pl.ds(r * share, share), :].astype(jnp.bfloat16)

        @pl.loop(1, n_ret)
        def _(k):
            part_copy(n, k).start()

        gathered[n, 0] = parts[n, me]

    @pl.loop(1, n_ret)
    def _(k):
        for n in range(tiles):
            part_copy(n, k).wait()


def step(shard_ids, row_ids, enc, w_key, w_value, queries, grad_out, n_ret, n_ctx):
    db_dev, length, width = enc.shape
    requests = shard_ids.shape[0] * shard_ids.shape[1]
    seq, feat = queries.shape
    rows = length // n_ctx
    half = width // 2
    padded = -(-half // n_ret // 16) * 16
    tiles = 2 * feat // PAIR
    hop_max = n_ctx // 2
    dma = pltpu.SemaphoreType.DMA
    bf16, vmem = jnp.bfloat16, pltpu.VMEM
    smem_spec = pl.BlockSpec(memory_space=pltpu.SMEM)
    any_spec = pl.BlockSpec(memory_space=pl.ANY)
    vmem_spec = pl.BlockSpec(memory_space=pltpu.VMEM)
    return pl.pallas_call(
        functools.partial(step_kernel, n_ret, n_ctx),
        out_shape=(
            jax.ShapeDtypeStruct((seq, feat), bf16),
            jax.ShapeDtypeStruct((seq, feat), bf16),
            jax.ShapeDtypeStruct((tiles, n_ret, padded, PAIR), bf16),
        ),
        in_specs=[smem_spec] * 2 + [any_spec] * 5,
        out_specs=(vmem_spec,) * 3,
        scratch_shapes=[
            vmem((n_ret, 1, 128), jnp.int32),
            vmem((n_ret, 1, 128), jnp.int32),
            pltpu.SMEM((n_ret, 1, 128), jnp.int32),
            vmem((db_dev, rows, width), bf16),
            vmem((n_ret, CAPACITY, rows, width), bf16),
            vmem((n_ret * CAPACITY, rows, width), bf16),
            vmem((n_ctx, requests, rows, width), bf16),
            vmem((width, 2 * feat), bf16),
            vmem((seq, feat), bf16),
            vmem((seq, feat), bf16),
            vmem((requests // CHUNKS * NEIGH_LEN, 2 * feat), bf16),
            vmem((2, half, requests * NEIGH_LEN), bf16),
            vmem((requests * NEIGH_LEN, 2 * feat), bf16),
            vmem((tiles, half, PAIR), bf16),
            vmem((tiles, half, PAIR), bf16),
            vmem((half, PAIR), jnp.float32),
            vmem((tiles, n_ret, padded, PAIR), bf16),
            dma((6,)),
            dma((n_ret,)), dma((n_ret,)),
            dma((n_ret,)), dma((n_ret,)),
            dma((2, CHUNKS, hop_max)), dma((2, CHUNKS, hop_max)),
            dma((tiles,)), dma((tiles,)),
            dma((tiles, n_ret)), dma((tiles, n_ret)),
        ],
        compiler_params=pltpu.CompilerParams(
            collective_id=0, has_side_effects=True, vmem_limit_bytes=VMEM_LIMIT
        ),
    )(shard_ids, row_ids, enc, w_key, w_value, queries, grad_out)


def finish_kernel(att_in, dq_in, gathered, att_ref, dq_ref, key_ref, value_ref):
    att_ref[...] = att_in[...]
    dq_ref[...] = dq_in[...]
    tiles, n_ret, _, cols = gathered.shape
    share = key_ref.shape[0]
    for n in range(tiles):
        total = gathered[n, 0, :share, :].astype(jnp.float32)
        for k in range(1, n_ret):
            total = total + gathered[n, k, :share, :].astype(jnp.float32)
        target = key_ref if n < tiles // 2 else value_ref
        target[:, pl.ds(n % (tiles // 2) * cols, cols)] = total


def finish(attended, grad_queries, gathered, share):
    vmem = pl.BlockSpec(memory_space=pltpu.VMEM)
    tiles, _, _, cols = gathered.shape
    grad = jax.ShapeDtypeStruct((share, tiles // 2 * cols), jnp.float32)
    like = jax.ShapeDtypeStruct(attended.shape, attended.dtype)
    return pl.pallas_call(
        finish_kernel,
        out_shape=(like, like, grad, grad),
        in_specs=[vmem] * 3,
        out_specs=(vmem,) * 4,
    )(attended, grad_queries, gathered)


def solution(mesh):
    n_ret, n_ctx = mesh.shape["ret"], mesh.shape["ctx"]

    def local(queries, enc_states, w_key, w_value, shard_ids, row_ids, grad_out):
        width = enc_states.shape[2]
        enc = enc_states[0].reshape(-1, NEIGH_LEN, width)
        attended, grad_queries, gathered = step(
            shard_ids[0].T, row_ids[0].T, enc, w_key, w_value, queries[0], grad_out[0], n_ret, n_ctx
        )
        attended, grad_queries, grad_key, grad_value = finish(
            attended, grad_queries, gathered, width // (2 * n_ret)
        )
        return attended[None], grad_queries[None], grad_key, grad_value

    spread = P("dp", "ret", "ctx")
    listed = P("dp", "ret", None)
    return jax.shard_map(
        local,
        mesh=mesh,
        in_specs=(spread, listed, P(None, "ctx"), P(None, "ctx"), listed, listed, spread),
        out_specs=(spread, spread, P(("dp", "ret"), "ctx"), P(("dp", "ret"), "ctx")),
        check_vma=False,
    )
```
